128 devices in a mesh: dp: 1, tp: 16 (over z, y), cp: 8 (over x, core).
Axes of the slice: x: 4, y: 4, z: 4, core: 2. Of those that a mesh axis runs over, the one named last changes fastest.
Arguments:
- x_in: bfloat16 [16384, 3072], P(('dp', 'cp', 'tp'))
- seg_ids: int32 [16384], P(('dp', 'cp', 'tp'))
- w_q: bfloat16 [3072, 16, 256], P(None, 'tp')
- w_k: bfloat16 [3072, 16, 256], P(None, 'tp')
- w_v: bfloat16 [3072, 16, 256], P(None, 'tp')
- w_o: bfloat16 [16, 256, 3072], P('tp')
Outputs:
- output: bfloat16 [16384, 3072], P(('dp', 'cp', 'tp'))
All inputs are finite; a program needn't handle non-finite values.
Results may differ from the reference program's by a relative error of at most 0.00482496.
Values are sent between devices in bfloat16 or wider.
A program may use at most 1 GiB of HBM per device.

```python
import jax
import jax.numpy as jnp
from jax import lax

CP = 8
PIECE = 1024
D = 3072
HEADS = 16
KV_HEADS = 16
HEAD = 256
DOCS = 6
QROWS = 64
SEQ = 2 * CP * PIECE
GROUP = HEADS // KV_HEADS


def row_positions():
    row_idx = jnp.arange(SEQ)
    owner_rank = row_idx // (2 * PIECE)
    within = row_idx % (2 * PIECE)
    return jnp.where(within < PIECE, owner_rank * PIECE + within, (2 * CP - 1 - owner_rank) * PIECE + within - PIECE)


def draw_segments(seg_key):
    half_len = SEQ // 2
    key_cut, key_gap = jax.random.split(seg_key)
    offsets = jax.random.permutation(key_cut, half_len - 1)[: DOCS - 1] + 1
    gap_start = jax.random.randint(key_gap, (), 0, half_len)
    cut_points = offsets + half_len * (offsets > gap_start).astype(jnp.int32)
    seq_pos = jnp.arange(SEQ)
    seg_seq = jnp.sum((seq_pos[:, None] >= cut_points[None, :]).astype(jnp.int32), axis=1)
    return seg_seq[row_positions()].astype(jnp.int32)


def setup_inputs(seed: int = 0, part: int = 0) -> dict:
    part_key = jax.random.fold_in(jax.random.key(seed), part)
    key_x, key_seg = jax.random.split(part_key)
    key_q, key_k, key_v, key_o = jax.random.split(jax.random.key(seed + 1), 4)
    x_in = jax.random.normal(key_x, (SEQ, D), jnp.float32).astype(jnp.bfloat16)
    seg_ids = draw_segments(key_seg)
    w_q = (jax.random.normal(key_q, (D, HEADS, HEAD), jnp.float32) * (1.5 * D ** -0.5)).astype(jnp.bfloat16)
    w_k = (jax.random.normal(key_k, (D, KV_HEADS, HEAD), jnp.float32) * D ** -0.5).astype(jnp.bfloat16)
    w_v = (jax.random.normal(key_v, (D, KV_HEADS, HEAD), jnp.float32) * D ** -0.5).astype(jnp.bfloat16)
    w_o = (jax.random.normal(key_o, (HEADS, HEAD, D), jnp.float32) * (4.0 * (HEADS * HEAD) ** -0.5)).astype(jnp.bfloat16)
    return {"x_in": x_in, "seg_ids": seg_ids, "w_q": w_q, "w_k": w_k, "w_v": w_v, "w_o": w_o}


def reference(x_in, seg_ids, w_q, w_k, w_v, w_o):
    pos_rows = row_positions()
    q_rows = jnp.dot(x_in, w_q.reshape(D, HEADS * HEAD), preferred_element_type=jnp.float32).astype(jnp.bfloat16)
    k_rows = jnp.dot(x_in, w_k.reshape(D, KV_HEADS * HEAD), preferred_element_type=jnp.float32).astype(jnp.bfloat16)
    v_rows = jnp.dot(x_in, w_v.reshape(D, KV_HEADS * HEAD), preferred_element_type=jnp.float32).astype(jnp.bfloat16)
    q_blocks = q_rows.reshape(SEQ // QROWS, QROWS, KV_HEADS, GROUP, HEAD).astype(jnp.float32)
    k_heads = k_rows.reshape(SEQ, KV_HEADS, HEAD).transpose(1, 0, 2).astype(jnp.float32)
    v_heads = v_rows.reshape(SEQ, KV_HEADS, HEAD).transpose(1, 0, 2).astype(jnp.float32)
    pos_blocks = pos_rows.reshape(SEQ // QROWS, QROWS)
    seg_blocks = seg_ids.reshape(SEQ // QROWS, QROWS)

    def query_block(blk_args):
        q_blk, pos_blk, seg_blk = blk_args
        visible = (seg_blk[:, None] == seg_ids[None, :]) & (pos_rows[None, :] <= pos_blk[:, None])

        def kv_head(head_args):
            q_head, k_head, v_head = head_args
            scores = jnp.einsum("qge,se->gqs", q_head, k_head) * HEAD ** -0.5
            scores = jnp.where(visible[None], scores, -jnp.inf)
            prob_rows = jnp.exp(scores - jnp.max(scores, axis=-1, keepdims=True))
            row_sum = jnp.sum(prob_rows, axis=-1)
            pv_sum = jnp.einsum("gqs,se->gqe", prob_rows.astype(jnp.bfloat16).astype(jnp.float32), v_head)
            return (pv_sum / row_sum[..., None]).astype(jnp.bfloat16)

        return lax.map(kv_head, (q_blk.transpose(1, 0, 2, 3), k_heads, v_heads))

    attn_rows = lax.map(query_block, (q_blocks, pos_blocks, seg_blocks))
    attn_rows = attn_rows.transpose(0, 3, 1, 2, 4).reshape(SEQ, HEADS * HEAD)
    y_out = jnp.dot(attn_rows, w_o.reshape(HEADS * HEAD, D), preferred_element_type=jnp.float32)
    return y_out.astype(jnp.bfloat16)
```

```python
import functools

import jax
import jax.numpy as jnp
from jax import lax
from jax.experimental import pallas as pl
from jax.experimental.pallas import tpu as pltpu
from jax.sharding import PartitionSpec as P

NEG_BIG = -1e30
LOG2E = 1.4426950408889634
N_DOCS = 6
SIDE = 4
MESH = pl.DeviceIdType.MESH

BATCHES = (
    ((0, 0, 0), (0, 0, 1)),
    ((0, 1, 0), (0, 3, 0), (1, 0, 1), (3, 0, 1)),
    ((1, 0, 0), (3, 0, 0), (0, 1, 1), (0, 3, 1)),
    ((0, 2, 0), (2, 0, 1), (1, 1, 0), (3, 1, 0), (1, 1, 1), (1, 3, 1)),
    ((1, 3, 0), (3, 3, 0), (3, 1, 1), (3, 3, 1), (2, 0, 0), (0, 2, 1)),
    ((1, 2, 0), (3, 2, 0), (2, 1, 1), (2, 3, 1), (2, 1, 0), (1, 2, 1)),
    ((2, 3, 0), (3, 2, 1), (2, 2, 0), (2, 2, 1)),
)
ORDER = tuple(blk for batch in BATCHES for blk in batch)


def gather_project_kernel(x_hbm, seg_ref, wq_hbm, wk_hbm, wv_hbm, q_ref, kv_hbm, cnt_ref,
                          x_buf, w_buf, kv_own, acc, cnt_mine, cnt_tp, cnt_row, cnt_cp,
                          send_sem, recv_sem, loc_sem, ctp_send, ctp_recv, ccp_send, ccp_recv):
    tp, cp = lax.axis_index("tp"), lax.axis_index("cp")
    n_tp, n_cp = SIDE * SIDE, 2 * SIDE
    z, y = lax.div(tp, SIDE), lax.rem(tp, SIDE)
    x, core = lax.div(cp, 2), lax.rem(cp, 2)
    half_rows = x_buf.shape[3]
    head_dim = q_ref.shape[-1]
    k_tile = 768
    n_used = [0]

    def at(pos, delta):
        return lax.rem(pos + delta, SIDE)

    def remote(src, dst, **device):
        idx = n_used[0]
        n_used[0] += 1
        return pltpu.make_async_remote_copy(src_ref=src, dst_ref=dst, send_sem=send_sem.at[idx], recv_sem=recv_sem.at[idx],
                                            device_id=device, device_id_type=MESH)

    sent = []

    def start(copies):
        for c in copies:
            c.start()
            sent.append(c)
        return copies

    def arrived(copies):
        for c in copies:
            c.wait_recv()

    load_x = pltpu.make_async_copy(x_hbm, x_buf.at[z, y], loc_sem.at[0])
    load_x.start()
    load_w = [pltpu.make_async_copy(w, w_buf.at[i], loc_sem.at[1 + i]) for i, w in enumerate((wq_hbm, wk_hbm, wv_hbm))]
    for c in load_w:
        c.start()
    cnt_mine[...] = (seg_ref[...] < lax.broadcasted_iota(jnp.int32, cnt_mine.shape, 0)).astype(jnp.int32)

    barrier = pltpu.get_barrier_semaphore()
    for d in range(1, n_tp):
        pl.semaphore_signal(barrier, inc=1, device_id={"tp": lax.rem(tp + d, n_tp)}, device_id_type=MESH)
    for d in range(1, n_cp):
        pl.semaphore_signal(barrier, inc=1, device_id={"cp": lax.rem(cp + d, n_cp)}, device_id_type=MESH)
    pl.semaphore_wait(barrier, n_tp - 1 + n_cp - 1)
    load_x.wait()

    def block(fam, b, a, lo=0, n=None):
        rows = pl.ds(lo, half_rows if n is None else n)
        return x_buf.at[b, a, 0, rows] if fam == 0 else x_buf.at[a, b, 1, rows]

    def my(fam):
        return (y, z) if fam == 0 else (z, y)

    def device_a(fam, delta):
        return z * SIDE + at(y, delta) if fam == 0 else at(z, delta) * SIDE + y

    def device_b(fam, delta):
        return device_a(1 - fam, delta)

    def first(fam):
        a, b = my(fam)
        return start([remote(block(fam, b, a), block(fam, b, a), tp=device_a(fam, d)) for d in (1, 3)])

    def first_forward(fam):
        a, b = my(fam)
        up, down = block(fam, b, at(a, 3), 0, half_rows // 2), block(fam, b, at(a, 1), half_rows // 2, half_rows // 2)
        return start([remote(up, up, tp=device_a(fam, 1)), remote(down, down, tp=device_a(fam, 3))])

    def second(fam, da):
        a, b = my(fam)
        src = block(fam, b, at(a, da))
        return start([remote(src, src, tp=device_b(fam, d)) for d in (1, 3)])

    def second_forward(fam, da):
        a, b = my(fam)
        up = block(fam, at(b, 3), at(a, da), 0, half_rows // 2)
        down = block(fam, at(b, 1), at(a, da), half_rows // 2, half_rows // 2)
        return start([remote(up, up, tp=device_b(fam, 1)), remote(down, down, tp=device_b(fam, 3))])

    def both(fn, *args):
        return fn(0, *args) + fn(1, *args)

    def project(i):
        blocks = [(at(z, dz), at(y, dy), h) for dz, dy, h in BATCHES[i]]
        rows = len(blocks) * half_rows
        off = sum(len(b) for b in BATCHES[:i]) * half_rows

        def k_step(kt, _):
            cols = pl.ds(pl.multiple_of(kt * k_tile, k_tile), k_tile)
            lhs = jnp.concatenate([x_buf[bz, by, h, :, cols] for bz, by, h in blocks], axis=0)
            for w in range(3):
                part = jnp.dot(lhs, w_buf[w, cols, :], preferred_element_type=jnp.float32)
                acc[w, :rows, :] = jnp.where(kt == 0, part, acc[w, :rows, :] + part)
            return 0

        lax.fori_loop(0, x_buf.shape[-1] // k_tile, k_step, 0)
        for n, (bz, by, h) in enumerate(blocks):
            q_ref[bz, by, h] = acc[0, n * half_rows:(n + 1) * half_rows, :].astype(jnp.bfloat16)
        kv_own[off:off + rows, :head_dim] = acc[1, :rows, :].astype(jnp.bfloat16)
        kv_own[off:off + rows, head_dim:] = acc[2, :rows, :].astype(jnp.bfloat16)
        return off, rows

    other = x * 2 + 1 - core

    def ring(delta):
        return at(x, delta) * 2 + core

    spans, kv_direct, kv_forward, kv_pair, kv_local = {}, {}, {}, [], []

    def kv_send(i, off, rows):
        span = pl.ds(off, rows)
        spans[i] = (off, rows)
        src, dst = kv_own.at[span], kv_hbm.at[cp, span]
        keep = pltpu.make_async_copy(src, dst, loc_sem.at[4 + i])
        keep.start()
        kv_local.append(keep)
        kv_direct[i] = start([remote(src, dst, cp=ring(1)), remote(src, dst, cp=ring(3))])
        kv_pair.extend(start([remote(src, dst, cp=other)]))

    def kv_relay(i):
        off, rows = spans[i]
        arrived(kv_direct[i])
        up, down = kv_hbm.at[ring(3), pl.ds(off, rows // 2)], kv_hbm.at[ring(1), pl.ds(off + rows // 2, rows // 2)]
        kv_forward[i] = start([remote(up, up, cp=ring(1)), remote(down, down, cp=ring(3))])
        for d in (3, 1):
            ref = kv_hbm.at[ring(d), pl.ds(off, rows)]
            kv_pair.extend(start([remote(ref, ref, cp=other)]))

    def kv_finish(i):
        off, rows = spans[i]
        arrived(kv_forward[i])
        ref = kv_hbm.at[ring(2), pl.ds(off, rows)]
        kv_pair.extend(start([remote(ref, ref, cp=other)]))

    s1 = both(first)
    s2 = {0: both(second, 0)}
    f2 = {}
    ctp = []
    for d in range(1, n_tp):
        c = pltpu.make_async_remote_copy(src_ref=cnt_mine, dst_ref=cnt_tp.at[d - 1], send_sem=ctp_send.at[d - 1], recv_sem=ctp_recv.at[d - 1],
                                         device_id={"tp": lax.rem(tp + d, n_tp)}, device_id_type=MESH)
        c.start()
        ctp.append(c)
    for c in load_w:
        c.wait()
    b0 = project(0)
    arrived(s1)
    f1 = both(first_forward)
    s2[1] = both(second, 1)
    s2[2] = both(second, 3)
    kv_send(0, *b0)
    total = cnt_mine[...]
    for d in range(1, n_tp):
        ctp[d - 1].wait_recv()
        total = total + cnt_tp[d - 1]
    cnt_row[...] = total
    b1 = project(1)
    ccp = []
    for d in range(1, n_cp):
        c = pltpu.make_async_remote_copy(src_ref=cnt_row, dst_ref=cnt_cp.at[d - 1], send_sem=ccp_send.at[d - 1], recv_sem=ccp_recv.at[d - 1],
                                         device_id={"cp": lax.rem(cp + d, n_cp)}, device_id_type=MESH)
        c.start()
        ccp.append(c)
    arrived(s2[0])
    f2[0] = both(second_forward, 0)
    kv_send(1, *b1)
    b2 = project(2)
    arrived(f1)
    s2[3] = both(second, 2)
    kv_relay(0)
    kv_send(2, *b2)
    arrived(s2[1])
    f2[1] = both(second_forward, 1)
    b3 = project(3)
    kv_relay(1)
    kv_finish(0)
    kv_send(3, *b3)
    arrived(s2[2])
    f2[2] = both(second_forward, 3)
    arrived(f2[0])
    b4 = project(4)
    kv_relay(2)
    kv_finish(1)
    kv_send(4, *b4)
    arrived(s2[3])
    f2[3] = both(second_forward, 2)
    arrived(f2[1])
    b5 = project(5)
    kv_relay(3)
    kv_finish(2)
    kv_send(5, *b5)
    arrived(f2[2])
    arrived(f2[3])
    b6 = project(6)
    kv_relay(4)
    kv_send(6, *b6)
    kv_finish(3)
    kv_relay(5)
    kv_finish(4)
    kv_relay(6)
    kv_finish(5)
    kv_finish(6)
    total = cnt_row[...]
    for d in range(1, n_cp):
        ccp[d - 1].wait_recv()
        total = total + cnt_cp[d - 1]
    cnt_ref[...] = total
    arrived(kv_pair)
    for c in sent + ctp + ccp:
        c.wait_send()
    for c in kv_local:
        c.wait()


N_REMOTE = 40 + 7 * 8


def gather_project(x_loc, seg_loc, w_q, w_k, w_v):
    rows, depth = x_loc.shape
    head_dim = w_q.shape[-1]
    half = rows // 2
    n_tp, n_cp = SIDE * SIDE, 2 * SIDE
    most = max(len(b) for b in BATCHES) * half
    any_spec = pl.BlockSpec(memory_space=pl.ANY)
    vmem_spec = pl.BlockSpec(memory_space=pltpu.VMEM)
    dma = pltpu.SemaphoreType.DMA
    q, kv, cnt = pl.pallas_call(
        gather_project_kernel,
        out_shape=(jax.ShapeDtypeStruct((SIDE, SIDE, 2, half, head_dim), jnp.bfloat16),
                   jax.ShapeDtypeStruct((n_cp, n_tp * rows, 2 * head_dim), jnp.bfloat16),
                   jax.ShapeDtypeStruct((8, rows), jnp.int32)),
        in_specs=[any_spec, vmem_spec, any_spec, any_spec, any_spec],
        out_specs=(vmem_spec, any_spec, vmem_spec),
        scratch_shapes=[pltpu.VMEM((SIDE, SIDE, 2, half, depth), jnp.bfloat16), pltpu.VMEM((3, depth, head_dim), jnp.bfloat16),
                        pltpu.VMEM((n_tp * rows, 2 * head_dim), jnp.bfloat16), pltpu.VMEM((3, most, head_dim), jnp.float32),
                        pltpu.VMEM((8, rows), jnp.int32), pltpu.VMEM((n_tp - 1, 8, rows), jnp.int32),
                        pltpu.VMEM((8, rows), jnp.int32), pltpu.VMEM((n_cp - 1, 8, rows), jnp.int32),
                        dma((N_REMOTE,)), dma((N_REMOTE,)), dma((4 + len(BATCHES),)),
                        dma((n_tp - 1,)), dma((n_tp - 1,)), dma((n_cp - 1,)), dma((n_cp - 1,))],
        compiler_params=pltpu.CompilerParams(collective_id=0, has_side_effects=True, vmem_limit_bytes=40 * 2**20),
        cost_estimate=pl.CostEstimate(flops=40 * 10**9, bytes_accessed=30 * 10**6, transcendentals=0),
        name="gather_project",
    )(x_loc.reshape(2, half, depth), seg_loc.reshape(1, rows), w_q, w_k, w_v)
    return q.reshape(n_tp * rows, head_dim), kv.reshape(n_cp * n_tp * rows, 2 * head_dim), jnp.sum(cnt, axis=1)


def flash_kernel(dims, starts, where_am, table, q_ref, kv_hbm, o_ref, kv_buf, m_buf, l_buf, acc_buf, sem):
    n_cp, piece, head_dim, half, tq, tk, nrow = dims
    r, z, y = where_am[0], where_am[1], where_am[2]
    n_pieces = 2 * n_cp
    coef = LOG2E * head_dim ** -0.5
    per_half = piece // half

    def doc_start(pos):
        lo = jnp.zeros_like(pos)
        for d in range(N_DOCS):
            lo = jnp.where(pos >= starts[d], jnp.maximum(lo, starts[d]), lo)
        return lo

    early0, late0 = r * piece, (n_pieces - 1 - r) * piece
    early_lo, late_lo = lax.div(doc_start(early0), piece), lax.div(doc_start(late0), piece)

    def needed(t):
        return ((t >= early_lo) & (t <= r)) | ((t >= late_lo) & (t <= n_pieces - 1 - r))

    def load(t, _):
        @pl.when(needed(t))
        def _():
            late = (t >= n_cp).astype(jnp.int32)
            owner = jnp.where(t >= n_cp, n_pieces - 1 - t, t)

            def one(i, _):
                bz, by, h = late * 2 + lax.div(i, 2 * SIDE), lax.rem(lax.div(i, 2), SIDE), lax.rem(i, 2)
                n = table[lax.rem(bz - z + SIDE, SIDE) * 2 * SIDE + lax.rem(by - y + SIDE, SIDE) * 2 + h]
                pltpu.make_async_copy(kv_hbm.at[pl.ds(pl.multiple_of(owner * 2 * piece + n * half, half), half)],
                                      kv_buf.at[pl.ds(pl.multiple_of(t * piece + i * half, half), half)], sem.at[t]).start()
                return 0

            lax.fori_loop(0, per_half, one, 0)
        return 0

    lax.fori_loop(0, n_pieces, load, 0)

    def settle(t, _):
        @pl.when(needed(t))
        def _():
            ref = kv_buf.at[pl.ds(pl.multiple_of(t * piece, piece), piece)]
            pltpu.make_async_copy(ref, ref, sem.at[t]).wait()
        return 0

    lax.fori_loop(0, r + 1, settle, 0)
    per_piece = piece // tq

    def q_step(qt, _):
        @pl.when(qt == per_piece)
        def _():
            lax.fori_loop(r + 1, n_pieces, settle, 0)
        row0 = pl.multiple_of(qt * tq, tq)
        p0 = jnp.where(qt < per_piece, early0 + row0, late0 + row0 - piece)
        lo0, lo1 = doc_start(p0), doc_start(p0 + tq - 1)
        j_lo, j_hi = lax.div(lo0, tk), lax.div(p0 + tq - 1, tk) + 1
        m_buf[...] = jnp.full_like(m_buf, NEG_BIG)
        l_buf[...] = jnp.zeros_like(l_buf)
        acc_buf[...] = jnp.zeros_like(acc_buf)

        def tile(k0, masked):
            k_blk = kv_buf[pl.ds(k0, tk), :head_dim]
            v_blk = kv_buf[pl.ds(k0, tk), head_dim:]
            for rc in range(tq // nrow):
                rows = pl.ds(rc * nrow, nrow)
                q_blk = q_ref[pl.ds(pl.multiple_of(row0 + rc * nrow, nrow), nrow), :]
                s = lax.dot_general(q_blk, k_blk, (((1,), (1,)), ((), ())), preferred_element_type=jnp.float32)
                if masked:
                    pos_q = p0 + rc * nrow + lax.broadcasted_iota(jnp.int32, (nrow, 128), 0)
                    lo_q = jnp.tile(doc_start(pos_q), (1, tk // 128))
                    pos_q = jnp.tile(pos_q, (1, tk // 128))
                    pos_k = k0 + lax.broadcasted_iota(jnp.int32, (nrow, tk), 1)
                    s = jnp.where((pos_k <= pos_q) & (pos_k >= lo_q), s, NEG_BIG)
                m_old = m_buf[rows, :]
                m_new = jnp.maximum(m_old, jnp.max(s, axis=1, keepdims=True))
                alpha = jnp.exp2((m_old - m_new) * coef)
                p = jnp.exp2((s - jnp.tile(m_new, (1, tk // 128))) * coef)
                l_new = alpha * l_buf[rows, :]
                for c in range(tk // 128):
                    l_new = l_new + p[:, c * 128:(c + 1) * 128]
                l_buf[rows, :] = l_new
                m_buf[rows, :] = m_new
                pv = jnp.dot(p.astype(jnp.bfloat16), v_blk, preferred_element_type=jnp.float32)
                acc_buf[rows, :] = acc_buf[rows, :] * jnp.tile(alpha, (1, head_dim // 128)) + pv

        def kv_step(j, _):
            k0 = pl.multiple_of(j * tk, tk)
            need = (k0 + tk - 1 > p0) | (k0 < lo1)
            pl.when(need)(lambda: tile(k0, True))
            pl.when(jnp.logical_not(need))(lambda: tile(k0, False))
            return 0

        lax.fori_loop(j_lo, j_hi, kv_step, 0)
        l_tot = jnp.sum(l_buf[...], axis=1, keepdims=True)
        o_ref[pl.ds(row0, tq), :] = (acc_buf[...] / l_tot).astype(jnp.bfloat16)
        return 0

    lax.fori_loop(0, 2 * per_piece, q_step, 0)


def flash(starts, where_am, q, kv, half, n_cp, tq=512, tk=1024, nrow=256):
    n_rows, head_dim = q.shape
    piece = n_rows // 2
    dims = (n_cp, piece, head_dim, half, tq, tk, nrow)
    table = [0] * len(ORDER)
    for n, (dz, dy, h) in enumerate(ORDER):
        table[dz * 2 * SIDE + dy * 2 + h] = n
    whole = pl.BlockSpec((n_rows, head_dim), lambda i, *_: (0, 0), pipeline_mode=pl.Buffered(1))
    gs = pltpu.PrefetchScalarGridSpec(
        num_scalar_prefetch=3, grid=(1,), in_specs=[whole, pl.BlockSpec(memory_space=pl.ANY)], out_specs=whole,
        scratch_shapes=[pltpu.VMEM(kv.shape, jnp.bfloat16), pltpu.VMEM((tq, 128), jnp.float32), pltpu.VMEM((tq, 128), jnp.float32),
                        pltpu.VMEM((tq, head_dim), jnp.float32), pltpu.SemaphoreType.DMA((2 * n_cp,))])
    return pl.pallas_call(
        functools.partial(flash_kernel, dims), out_shape=jax.ShapeDtypeStruct((n_rows, head_dim), jnp.bfloat16),
        grid_spec=gs, name="flash", compiler_params=pltpu.CompilerParams(vmem_limit_bytes=40 * 2**20),
        cost_estimate=pl.CostEstimate(flops=20 * 10**9, bytes_accessed=20 * 10**6, transcendentals=0),
    )(starts, where_am, jnp.array(table, jnp.int32), q, kv)


def solution(mesh):
    n_tp, n_cp = mesh.shape["tp"], mesh.shape["cp"]
    pair_perm = [(i, i ^ 1) for i in range(n_cp)]

    def per_device(x_loc, seg_loc, w_q, w_k, w_v, w_o):
        tp, cp = lax.axis_index("tp"), lax.axis_index("cp")
        core = lax.rem(cp, 2)
        rows, depth = x_loc.shape
        head_dim = w_q.shape[-1]
        q, kv, starts = gather_project(x_loc, seg_loc, w_q.reshape(depth, head_dim), w_k.reshape(depth, head_dim), w_v.reshape(depth, head_dim))
        wide = w_o.shape[-1] // 2
        wo_part = lax.dynamic_slice(w_o.reshape(head_dim, 2 * wide), (0, core * wide), (head_dim, wide))
        wo_part, kv = lax.optimization_barrier((wo_part, kv))
        wo_half = lax.all_gather(wo_part, "tp", axis=0, tiled=True)
        where_am = jnp.stack([cp, lax.div(tp, SIDE), lax.rem(tp, SIDE)]).astype(jnp.int32)
        o = flash(starts, where_am, q, kv, rows // 2, n_cp)
        o_heads = lax.all_to_all(o.reshape(n_tp, rows, head_dim), "tp", 0, 0, tiled=False)
        o_rows = o_heads.transpose(1, 0, 2).reshape(rows, n_tp * head_dim)
        o_pair = lax.ppermute(o_rows, "cp", pair_perm)
        both = jnp.concatenate([o_rows, o_pair], axis=0)
        y_both = jnp.dot(both, wo_half, preferred_element_type=jnp.float32).astype(jnp.bfloat16)
        y_mine, y_pair = y_both[:rows], lax.ppermute(y_both[rows:], "cp", pair_perm)
        return jnp.where(core == 0, jnp.concatenate([y_mine, y_pair], axis=1), jnp.concatenate([y_pair, y_mine], axis=1))

    return jax.shard_map(
        per_device, mesh=mesh,
        in_specs=(P(("dp", "cp", "tp"), None), P(("dp", "cp", "tp")), P(None, "tp", None), P(None, "tp", None), P(None, "tp", None), P("tp", None, None)),
        out_specs=P(("dp", "cp", "tp"), None), check_vma=False)
```

```python
import jax
import jax.numpy as jnp
from jax import lax
from jax.experimental import pallas as pl
from jax.experimental.pallas import tpu as pltpu
from jax.sharding import PartitionSpec as P

NEG_BIG = -1e30
LOG2E = 1.4426950408889634
N_DOCS = 6
SIDE = 4
MESH = pl.DeviceIdType.MESH

BATCHES = (
    ((0, 0, 0), (0, 0, 1)),
    ((0, 1, 0), (0, 3, 0), (1, 0, 1), (3, 0, 1)),
    ((1, 0, 0), (3, 0, 0), (0, 1, 1), (0, 3, 1)),
    ((0, 2, 0), (2, 0, 1), (1, 1, 0), (3, 1, 0), (1, 1, 1), (1, 3, 1)),
    ((1, 3, 0), (3, 3, 0), (3, 1, 1), (3, 3, 1), (2, 0, 0), (0, 2, 1)),
    ((1, 2, 0), (3, 2, 0), (2, 1, 1), (2, 3, 1), (2, 1, 0), (1, 2, 1)),
    ((2, 3, 0), (3, 2, 1), (2, 2, 0), (2, 2, 1)),
)
ORDER = tuple(blk for batch in BATCHES for blk in batch)


def attention_kernel(x_hbm, seg_ref, wq_hbm, wk_hbm, wv_hbm, wo_hbm, y_hbm, kv_hbm,
                     x_buf, w_buf, kv_own, acc, q_buf, stage, m_buf, l_buf, o_acc, lo_buf, wo_buf, o_mine, o_all, y_acc, y_out,
                     cnt_mine, cnt_tp, cnt_row, cnt_cp, send_sem, recv_sem, loc_sem, stage_sem):
    tp, cp = lax.axis_index("tp"), lax.axis_index("cp")
    n_tp, n_cp = SIDE * SIDE, 2 * SIDE
    z, y = lax.div(tp, SIDE), lax.rem(tp, SIDE)
    x, core = lax.div(cp, 2), lax.rem(cp, 2)
    other = x * 2 + 1 - core
    half_rows = x_buf.shape[3]
    head_dim = q_buf.shape[-1]
    n_rows = q_buf.shape[0]
    piece = n_rows // 2
    n_pieces = 2 * n_cp
    wide = wo_buf.shape[-1]
    coef = LOG2E * head_dim ** -0.5
    k_tile = 768
    n_used = [0]

    def at(pos, delta):
        return lax.rem(pos + delta, SIDE)

    def remote(src, dst, **device):
        idx = n_used[0]
        n_used[0] += 1
        return pltpu.make_async_remote_copy(src_ref=src, dst_ref=dst, send_sem=send_sem.at[idx], recv_sem=recv_sem.at[idx],
                                            device_id=device, device_id_type=MESH)

    sent = []

    def start(copies):
        for c in copies:
            c.start()
            sent.append(c)
        return copies

    def arrived(copies):
        for c in copies:
            c.wait_recv()

    load_x = pltpu.make_async_copy(x_hbm, x_buf.at[z, y], loc_sem.at[0])
    load_x.start()
    load_w = [pltpu.make_async_copy(w, w_buf.at[i], loc_sem.at[1 + i]) for i, w in enumerate((wq_hbm, wk_hbm, wv_hbm))]
    for c in load_w:
        c.start()
    load_wo = pltpu.make_async_copy(wo_hbm.at[:, :, pl.ds(pl.multiple_of(core * wide, wide), wide)], wo_buf.at[z, y], loc_sem.at[4])
    load_wo.start()
    cnt_mine[...] = (seg_ref[...] < lax.broadcasted_iota(jnp.int32, cnt_mine.shape, 0)).astype(jnp.float32)

    barrier = pltpu.get_barrier_semaphore()
    for d in range(1, n_tp):
        pl.semaphore_signal(barrier, inc=1, device_id={"tp": lax.rem(tp + d, n_tp)}, device_id_type=MESH)
    for d in range(1, n_cp):
        pl.semaphore_signal(barrier, inc=1, device_id={"cp": lax.rem(cp + d, n_cp)}, device_id_type=MESH)
    pl.semaphore_wait(barrier, n_tp - 1 + n_cp - 1)
    load_x.wait()

    def device_a(fam, delta):
        return z * SIDE + at(y, delta) if fam == 0 else at(z, delta) * SIDE + y

    def device_b(fam, delta):
        return device_a(1 - fam, delta)

    class Plane:
        def __init__(self, buf):
            self.buf = buf
            self.rows = buf.shape[3]
            self.s1, self.f1, self.s2, self.f2 = [], [], {}, {}

        def block(self, fam, b, a, part=None):
            half = self.rows // 2
            rows = pl.ds(0, self.rows) if part is None else pl.ds(part * half, half)
            return self.buf.at[b, a, 0, rows] if fam == 0 else self.buf.at[a, b, 1, rows]

        def first(self):
            for fam, (a, b) in enumerate(((y, z), (z, y))):
                src = self.block(fam, b, a)
                self.s1 += start([remote(src, src, tp=device_a(fam, d)) for d in (1, 3)])

        def first_forward(self):
            arrived(self.s1)
            for fam, (a, b) in enumerate(((y, z), (z, y))):
                up, down = self.block(fam, b, at(a, 3), 0), self.block(fam, b, at(a, 1), 1)
                self.f1 += start([remote(up, up, tp=device_a(fam, 1)), remote(down, down, tp=device_a(fam, 3))])

        def second(self, da):
            self.s2[da] = []
            for fam, (a, b) in enumerate(((y, z), (z, y))):
                src = self.block(fam, b, at(a, da))
                self.s2[da] += start([remote(src, src, tp=device_b(fam, d)) for d in (1, 3)])

        def second_forward(self, da):
            arrived(self.s2[da])
            self.f2[da] = []
            for fam, (a, b) in enumerate(((y, z), (z, y))):
                up, down = self.block(fam, at(b, 3), at(a, da), 0), self.block(fam, at(b, 1), at(a, da), 1)
                self.f2[da] += start([remote(up, up, tp=device_b(fam, 1)), remote(down, down, tp=device_b(fam, 3))])

    xs, ws = Plane(x_buf), Plane(wo_buf)

    def project(i):
        blocks = [(at(z, dz), at(y, dy), h) for dz, dy, h in BATCHES[i]]
        rows = len(blocks) * half_rows
        off = sum(len(b) for b in BATCHES[:i]) * half_rows

        def k_step(kt, _):
            cols = pl.ds(pl.multiple_of(kt * k_tile, k_tile), k_tile)
            lhs = jnp.concatenate([x_buf[bz, by, h, :, cols] for bz, by, h in blocks], axis=0)
            for w in range(3):
                part = jnp.dot(lhs, w_buf[w, cols, :], preferred_element_type=jnp.float32)
                acc[w, :rows, :] = jnp.where(kt == 0, part, acc[w, :rows, :] + part)
            return 0

        lax.fori_loop(0, x_buf.shape[-1] // k_tile, k_step, 0)
        for n, (bz, by, h) in enumerate(blocks):
            span = slice(n * half_rows, (n + 1) * half_rows)
            row = pl.ds(pl.multiple_of(((bz * SIDE + by) * 2 + h) * half_rows, half_rows), half_rows)
            q_buf[row, :] = acc[0, span, :].astype(jnp.bfloat16)
            k_new, v_new = acc[1, span, :].astype(jnp.bfloat16), acc[2, span, :].astype(jnp.bfloat16)
            stage[0, row, :head_dim] = k_new
            stage[0, row, head_dim:] = v_new
            kv_own[off + n * half_rows:off + (n + 1) * half_rows, :head_dim] = k_new
            kv_own[off + n * half_rows:off + (n + 1) * half_rows, head_dim:] = v_new
        spans[i] = (off, rows)

    def ring(delta):
        return at(x, delta) * 2 + core

    spans, kv_direct, kv_forward, pair_own, pair_side, pair_far = {}, {}, {}, [], [], []

    def kv_send(i):
        span = pl.ds(*spans[i])
        src, dst = kv_own.at[span], kv_hbm.at[cp, span]
        kv_direct[i] = start([remote(src, dst, cp=ring(1)), remote(src, dst, cp=ring(3))])
        pair_own.extend(start([remote(src, dst, cp=other)]))

    def kv_relay(i):
        off, rows = spans[i]
        arrived(kv_direct[i])
        up, down = kv_hbm.at[ring(3), pl.ds(off, rows // 2)], kv_hbm.at[ring(1), pl.ds(off + rows // 2, rows // 2)]
        kv_forward[i] = start([remote(up, up, cp=ring(1)), remote(down, down, cp=ring(3))])
        for d in (3, 1):
            ref = kv_hbm.at[ring(d), pl.ds(off, rows)]
            pair_side.extend(start([remote(ref, ref, cp=other)]))

    def kv_finish(i):
        arrived(kv_forward[i])
        ref = kv_hbm.at[ring(2), pl.ds(*spans[i])]
        pair_far.extend(start([remote(ref, ref, cp=other)]))

    xs.first()
    xs.second(0)
    ctp = start([remote(cnt_mine, cnt_tp.at[d - 1], tp=lax.rem(tp + d, n_tp)) for d in range(1, n_tp)])
    for c in load_w:
        c.wait()
    project(0)
    xs.first_forward()
    xs.second(1)
    xs.second(3)
    kv_send(0)
    arrived(ctp)
    total = cnt_mine[...]
    for d in range(1, n_tp):
        total = total + cnt_tp[d - 1]
    cnt_row[...] = total
    project(1)
    ccp = start([remote(cnt_row, cnt_cp.at[d - 1], cp=lax.rem(cp + d, n_cp)) for d in range(1, n_cp)])
    xs.second_forward(0)
    kv_send(1)
    project(2)
    arrived(xs.f1)
    xs.second(2)
    kv_relay(0)
    kv_send(2)
    xs.second_forward(1)
    project(3)
    kv_relay(1)
    kv_finish(0)
    kv_send(3)
    xs.second_forward(3)
    arrived(xs.f2[0])
    project(4)
    kv_relay(2)
    kv_finish(1)
    kv_send(4)
    xs.second_forward(2)
    load_wo.wait()
    ws.first()
    ws.second(0)
    arrived(xs.f2[1])
    project(5)
    kv_relay(3)
    kv_finish(2)
    kv_send(5)
    arrived(xs.f2[3])
    arrived(xs.f2[2])
    project(6)
    kv_relay(4)
    kv_send(6)
    kv_finish(3)

    arrived(ccp)
    total = cnt_row[...]
    for d in range(1, n_cp):
        total = total + cnt_cp[d - 1]
    bounds = jnp.sum(total, axis=1, keepdims=True)
    n_part = 256

    def position(row0):
        late = lax.div(row0, piece)
        return (1 - late) * (cp * piece + row0) + late * ((n_pieces - 1 - cp) * piece + row0 - piece)

    def prepare(i, _):
        row0 = pl.multiple_of(i * n_part, n_part)
        pos = (position(row0) + lax.broadcasted_iota(jnp.int32, (n_part, 128), 0)).astype(jnp.float32)
        lo = jnp.zeros_like(pos)
        for d in range(N_DOCS):
            begin = jnp.broadcast_to(bounds[d:d + 1, :], pos.shape)
            lo = jnp.where(pos >= begin, jnp.maximum(lo, begin), lo)
        rows = pl.ds(row0, n_part)
        lo_buf[rows, :] = lo.astype(jnp.int32)
        m_buf[rows, :] = jnp.full((n_part, 128), NEG_BIG, jnp.float32)
        l_buf[rows, :] = jnp.zeros((n_part, 128), jnp.float32)
        o_acc[rows, :] = jnp.zeros((n_part, head_dim), jnp.float32)
        return 0

    lax.fori_loop(0, n_rows // n_part, prepare, 0)

    def attend(slot, row0, key_tile, pos_k0, causal):
        keys = pl.ds(pl.multiple_of(key_tile * piece, piece), piece)
        k_blk = stage[slot, keys, :head_dim]
        v_blk = stage[slot, keys, head_dim:]
        chains = [pl.ds(pl.multiple_of(row0 + c * CHAIN, CHAIN), CHAIN) for c in range(PAIR // CHAIN)]
        lane = lax.broadcasted_iota(jnp.int32, (CHAIN, piece), 1)
        wide_of = lambda v: jnp.tile(v, (1, piece // 128))
        scores = [lax.dot_general(q_buf[rows, :], k_blk, (((1,), (1,)), ((), ())), preferred_element_type=jnp.float32) for rows in chains]
        olds = [(m_buf[rows, :], l_buf[rows, :], o_acc[rows, :], lo_buf[rows, :]) for rows in chains]
        news = []
        for c, (s, (m_old, l_old, o_old, lo)) in enumerate(zip(scores, olds)):
            visible = lane >= wide_of(lo - pos_k0)
            if causal:
                pos_q = position(row0) + c * CHAIN - pos_k0 + lax.broadcasted_iota(jnp.int32, (CHAIN, 128), 0)
                visible = visible & (lane <= wide_of(pos_q))
            s = jnp.where(visible, s, NEG_BIG)
            m_new = jnp.maximum(m_old, jnp.max(s, axis=1, keepdims=True))
            alpha = jnp.exp2((m_old - m_new) * coef)
            p = jnp.exp2((s - wide_of(m_new)) * coef)
            l_new = alpha * l_old
            for i in range(piece // 128):
                l_new = l_new + p[:, i * 128:(i + 1) * 128]
            pv = jnp.dot(p.astype(jnp.bfloat16), v_blk, preferred_element_type=jnp.float32)
            news.append((m_new, l_new, o_old * jnp.tile(alpha, (1, head_dim // 128)) + pv))
        for rows, (m_new, l_new, o_new) in zip(chains, news):
            m_buf[rows, :] = m_new
            l_buf[rows, :] = l_new
            o_acc[rows, :] = o_new

    per_piece = piece // PAIR

    def diagonal(lo, hi):
        def step(u, _):
            key_tile = lax.div(u, 2 * per_piece)
            row0 = (u - key_tile * per_piece) * PAIR
            pos_k0 = (1 - key_tile) * cp * piece + key_tile * (n_pieces - 1 - cp) * piece
            attend(0, row0, key_tile, pos_k0, True)
            return 0
        lax.fori_loop(lo, hi, step, 0)

    def block_of(src, slot):
        earlier = lax.div(cp - src + n_cp - 1, n_cp)

        def step(u, _):
            key_tile = (1 - earlier) * lax.div(u, per_piece)
            row0 = (earlier * u + (1 - earlier) * (per_piece + lax.rem(u, per_piece))) * PAIR
            pos_k0 = (1 - key_tile) * src * piece + key_tile * (n_pieces - 1 - src) * piece
            attend(slot, row0, key_tile, pos_k0, False)
            return 0
        lax.fori_loop(0, 2 * per_piece, step, 0)

    def fetch(src, slot):
        copies = []
        for n, (dz, dy, h) in enumerate(ORDER):
            row = pl.multiple_of(((at(z, dz) * SIDE + at(y, dy)) * 2 + h) * half_rows, half_rows)
            copies.append(pltpu.make_async_copy(kv_hbm.at[src, pl.ds(n * half_rows, half_rows)], stage.at[slot, pl.ds(row, half_rows)], stage_sem.at[slot]))
        for c in copies:
            c.start()
        return pltpu.make_async_copy(kv_hbm.at[src], stage.at[slot], stage_sem.at[slot])

    def landed(whole):
        whole.wait()

    n_diag = 3 * per_piece
    diagonal(0, n_diag // 3)
    kv_relay(5)
    kv_finish(4)
    diagonal(n_diag // 3, 2 * n_diag // 3)
    kv_relay(6)
    kv_finish(5)
    ws.first_forward()
    ws.second(1)
    ws.second(3)
    arrived(pair_own)
    now = fetch(other, 1)
    diagonal(2 * n_diag // 3, n_diag)
    kv_finish(6)
    ws.second_forward(0)

    def near(d, mine):
        return at(x, d) * 2 + (core if mine else 1 - core)

    landed(now)
    now = fetch(near(3, True), 0)
    block_of(other, 1)
    landed(now)
    now = fetch(near(1, True), 1)
    block_of(near(3, True), 0)
    arrived(ws.f1)
    ws.second(2)
    arrived(pair_side)
    landed(now)
    now = fetch(near(3, False), 0)
    block_of(near(1, True), 1)
    ws.second_forward(1)
    landed(now)
    now = fetch(near(1, False), 1)
    block_of(near(3, False), 0)
    ws.second_forward(3)
    landed(now)
    now = fetch(near(2, True), 0)
    block_of(near(1, False), 1)
    arrived(pair_far)
    landed(now)
    now = fetch(near(2, False), 1)
    block_of(near(2, True), 0)
    ws.second_forward(2)
    landed(now)
    block_of(near(2, False), 1)

    def finish(i, _):
        rows = pl.ds(pl.multiple_of(i * 128, 128), 128)
        o_mine[i] = (o_acc[rows, :] / jnp.sum(l_buf[rows, :], axis=1, keepdims=True)).astype(jnp.bfloat16)
        return 0

    lax.fori_loop(0, n_tp, finish, 0)
    turns = (0, 1, 3, 2)
    o_sent = {}
    for dz in turns:
        for dy in turns:
            if dz or dy:
                peer = at(z, dz) * SIDE + at(y, dy)
                o_sent[dz, dy] = start([remote(o_mine.at[peer], o_all.at[tp, 0], tp=peer)])
    o_pair = {(0, 0): start([remote(o_mine.at[tp], o_all.at[tp, 1], cp=other)])}
    o_all[tp, 0] = o_mine[tp]
    for turn, dz in enumerate(turns):
        for dy in turns:
            if dz or dy:
                arrived(o_sent[dz, dy])
                src = at(z, SIDE - dz) * SIDE + at(y, SIDE - dy)
                o_pair[dz, dy] = start([remote(o_all.at[src, 0], o_all.at[src, 1], cp=other)])
    for da in turns:
        arrived(ws.f2[da])
    for turn, dz in enumerate(turns):
        for dy in turns:
            arrived(o_pair[dz, dy])
        zz = at(z, SIDE - dz)

        def column(j, _):
            cols = pl.ds(pl.multiple_of(j * 512, 512), 512)
            lhs = jnp.concatenate([o_all[zz * SIDE + yy].reshape(2 * o_mine.shape[1], head_dim) for yy in range(SIDE)], axis=1)
            rhs = wo_buf[zz, :, :, :, cols].reshape(SIDE * head_dim, 512)
            part = jnp.dot(lhs, rhs, preferred_element_type=jnp.float32)
            y_acc[:, cols] = part if turn == 0 else y_acc[:, cols] + part
            return 0

        lax.fori_loop(0, wide // 512, column, 0)
    y_out[...] = y_acc[...].astype(jnp.bfloat16)
    rows = o_mine.shape[1]
    cols = pl.ds(pl.multiple_of(core * wide, wide), wide)
    keep = pltpu.make_async_copy(y_out.at[pl.ds(0, rows)], y_hbm.at[:, cols], loc_sem.at[5])
    keep.start()
    y_pair = start([remote(y_out.at[pl.ds(rows, rows)], y_hbm.at[:, cols], cp=other)])
    arrived(y_pair)
    keep.wait()
    for c in sent:
        c.wait_send()


N_REMOTE = 2 * 40 + 7 * 8 + 15 + 7 + 15 + 16 + 1
CHAIN = 256
PAIR = 512


def solution(mesh):
    def per_device(x_loc, seg_loc, w_q, w_k, w_v, w_o):
        rows, depth = x_loc.shape
        head_dim = w_q.shape[-1]
        half = rows // 2
        n_tp, n_cp = SIDE * SIDE, 2 * SIDE
        n_rows = n_tp * rows
        wide = w_o.shape[-1] // 2
        most = max(len(b) for b in BATCHES) * half
        hbm = pl.BlockSpec(memory_space=pltpu.HBM)
        f32, bf16 = jnp.float32, jnp.bfloat16
        dma, vmem = pltpu.SemaphoreType.DMA, pltpu.VMEM
        y_loc, _ = pl.pallas_call(
            attention_kernel,
            out_shape=(jax.ShapeDtypeStruct((rows, depth), bf16), jax.ShapeDtypeStruct((n_cp, n_rows, 2 * head_dim), bf16)),
            in_specs=[hbm, pl.BlockSpec(memory_space=vmem), hbm, hbm, hbm, hbm],
            out_specs=(hbm, hbm),
            scratch_shapes=[vmem((SIDE, SIDE, 2, half, depth), bf16), vmem((3, depth, head_dim), bf16),
                            vmem((n_rows, 2 * head_dim), bf16), vmem((3, most, head_dim), f32),
                            vmem((n_rows, head_dim), bf16), vmem((2, n_rows, 2 * head_dim), bf16),
                            vmem((n_rows, 128), f32), vmem((n_rows, 128), f32), vmem((n_rows, head_dim), f32),
                            vmem((n_rows, 128), jnp.int32), vmem((SIDE, SIDE, 2, head_dim // 2, wide), bf16),
                            vmem((n_tp, rows, head_dim), bf16), vmem((n_tp, 2, rows, head_dim), bf16),
                            vmem((2 * rows, wide), f32), vmem((2 * rows, wide), bf16),
                            vmem((8, rows), f32), vmem((n_tp - 1, 8, rows), f32), vmem((8, rows), f32), vmem((n_cp - 1, 8, rows), f32),
                            dma((N_REMOTE,)), dma((N_REMOTE,)), dma((6,)), dma((2,))],
            compiler_params=pltpu.CompilerParams(collective_id=0, has_side_effects=True, vmem_limit_bytes=63 * 2**20),
            cost_estimate=pl.CostEstimate(flops=40 * 10**9, bytes_accessed=30 * 10**6, transcendentals=0),
            name="packed_attention",
        )(x_loc.reshape(2, half, depth), seg_loc.reshape(1, rows), w_q.reshape(depth, head_dim), w_k.reshape(depth, head_dim),
          w_v.reshape(depth, head_dim), w_o.reshape(2, head_dim // 2, 2 * wide))
        return y_loc

    return jax.shard_map(
        per_device, mesh=mesh,
        in_specs=(P(("dp", "cp", "tp"), None), P(("dp", "cp", "tp")), P(None, "tp", None), P(None, "tp", None), P(None, "tp", None), P("tp", None, None)),
        out_specs=P(("dp", "cp", "tp"), None), check_vma=False)
```

```python
import jax
import jax.numpy as jnp
from jax import lax
from jax.experimental import pallas as pl
from jax.experimental.pallas import tpu as pltpu
from jax.sharding import PartitionSpec as P

NEG_BIG = -1e30
LOG2E = 1.4426950408889634
N_DOCS = 6
SIDE = 4
MESH = pl.DeviceIdType.MESH

BATCHES = (
    ((0, 0, 0), (0, 0, 1)),
    ((0, 1, 0), (0, 3, 0), (1, 0, 1), (3, 0, 1)),
    ((1, 0, 0), (3, 0, 0), (0, 1, 1), (0, 3, 1)),
    ((0, 2, 0), (2, 0, 1), (1, 1, 0), (3, 1, 0), (1, 1, 1), (1, 3, 1)),
    ((1, 3, 0), (3, 3, 0), (3, 1, 1), (3, 3, 1), (2, 0, 0), (0, 2, 1)),
    ((1, 2, 0), (3, 2, 0), (2, 1, 1), (2, 3, 1), (2, 1, 0), (1, 2, 1)),
    ((2, 3, 0), (3, 2, 1), (2, 2, 0), (2, 2, 1)),
)
ORDER = tuple(blk for batch in BATCHES for blk in batch)


def attention_kernel(x_hbm, seg_ref, wq_hbm, wk_hbm, wv_hbm, wo_hbm, y_hbm, kv_hbm,
                     x_buf, w_buf, kv_own, acc, q_buf, stage, m_buf, l_buf, o_acc, lo_buf, wo_buf, wx_buf, o_mine, o_all, y_acc, y_out,
                     cnt_mine, cnt_tp, cnt_row, cnt_cp, send_sem, recv_sem, loc_sem, stage_sem):
    tp, cp = lax.axis_index("tp"), lax.axis_index("cp")
    n_tp, n_cp = SIDE * SIDE, 2 * SIDE
    z, y = lax.div(tp, SIDE), lax.rem(tp, SIDE)
    x, core = lax.div(cp, 2), lax.rem(cp, 2)
    other = x * 2 + 1 - core
    half_rows = x_buf.shape[3]
    head_dim = q_buf.shape[-1]
    n_rows = q_buf.shape[0]
    piece = n_rows // 2
    n_pieces = 2 * n_cp
    n_plane, n_quarter = wo_buf.shape[-1], wx_buf.shape[-1]
    wide = n_plane + SIDE * n_quarter
    coef = LOG2E * head_dim ** -0.5
    k_tile = 768
    n_used = [0]

    def at(pos, delta):
        return lax.rem(pos + delta, SIDE)

    def remote(src, dst, **device):
        idx = n_used[0]
        n_used[0] += 1
        return pltpu.make_async_remote_copy(src_ref=src, dst_ref=dst, send_sem=send_sem.at[idx], recv_sem=recv_sem.at[idx],
                                            device_id=device, device_id_type=MESH)

    sent = []

    def start(copies):
        for c in copies:
            c.start()
            sent.append(c)
        return copies

    def arrived(copies):
        for c in copies:
            c.wait_recv()

    load_x = pltpu.make_async_copy(x_hbm, x_buf.at[z, y], loc_sem.at[0])
    load_x.start()
    load_w = [pltpu.make_async_copy(w, w_buf.at[i], loc_sem.at[1 + i]) for i, w in enumerate((wq_hbm, wk_hbm, wv_hbm))]
    for c in load_w:
        c.start()
    load_wo = [pltpu.make_async_copy(wo_hbm.at[:, :, pl.ds(pl.multiple_of(core * wide + first, n_quarter), size)], dst, loc_sem.at[4 + i])
               for i, (first, size, dst) in enumerate(((0, n_plane, wo_buf.at[z, y]), (n_plane + x * n_quarter, n_quarter, wx_buf.at[x, z, y])))]
    for c in load_wo:
        c.start()
    cnt_mine[...] = (seg_ref[...] < lax.broadcasted_iota(jnp.int32, cnt_mine.shape, 0)).astype(jnp.float32)

    barrier = pltpu.get_barrier_semaphore()
    for d in range(1, n_tp):
        pl.semaphore_signal(barrier, inc=1, device_id={"tp": lax.rem(tp + d, n_tp)}, device_id_type=MESH)
    for d in range(1, n_cp):
        pl.semaphore_signal(barrier, inc=1, device_id={"cp": lax.rem(cp + d, n_cp)}, device_id_type=MESH)
    pl.semaphore_wait(barrier, n_tp - 1 + n_cp - 1)
    load_x.wait()

    def device_a(fam, delta):
        return z * SIDE + at(y, delta) if fam == 0 else at(z, delta) * SIDE + y

    def device_b(fam, delta):
        return device_a(1 - fam, delta)

    class Plane:
        def __init__(self, buf):
            self.buf = buf
            self.rows = buf.shape[3]
            self.s1, self.f1, self.s2, self.f2 = [], [], {}, {}

        def block(self, fam, b, a, part=None):
            half = self.rows // 2
            rows = pl.ds(0, self.rows) if part is None else pl.ds(part * half, half)
            return self.buf.at[b, a, 0, rows] if fam == 0 else self.buf.at[a, b, 1, rows]

        def first(self):
            for fam, (a, b) in enumerate(((y, z), (z, y))):
                src = self.block(fam, b, a)
                self.s1 += start([remote(src, src, tp=device_a(fam, d)) for d in (1, 3)])

        def first_forward(self):
            arrived(self.s1)
            for fam, (a, b) in enumerate(((y, z), (z, y))):
                up, down = self.block(fam, b, at(a, 3), 0), self.block(fam, b, at(a, 1), 1)
                self.f1 += start([remote(up, up, tp=device_a(fam, 1)), remote(down, down, tp=device_a(fam, 3))])

        def second(self, da):
            self.s2[da] = []
            for fam, (a, b) in enumerate(((y, z), (z, y))):
                src = self.block(fam, b, at(a, da))
                self.s2[da] += start([remote(src, src, tp=device_b(fam, d)) for d in (1, 3)])

        def second_forward(self, da):
            arrived(self.s2[da])
            self.f2[da] = []
            for fam, (a, b) in enumerate(((y, z), (z, y))):
                up, down = self.block(fam, at(b, 3), at(a, da), 0), self.block(fam, at(b, 1), at(a, da), 1)
                self.f2[da] += start([remote(up, up, tp=device_b(fam, 1)), remote(down, down, tp=device_b(fam, 3))])

    xs, ws, wq = Plane(x_buf), Plane(wo_buf), Plane(wx_buf.at[x])

    def project(i):
        blocks = [(at(z, dz), at(y, dy), h) for dz, dy, h in BATCHES[i]]
        rows = len(blocks) * half_rows
        off = sum(len(b) for b in BATCHES[:i]) * half_rows

        def k_step(kt, _):
            cols = pl.ds(pl.multiple_of(kt * k_tile, k_tile), k_tile)
            lhs = jnp.concatenate([x_buf[bz, by, h, :, cols] for bz, by, h in blocks], axis=0)
            for w in range(3):
                part = jnp.dot(lhs, w_buf[w, cols, :], preferred_element_type=jnp.float32)
                acc[w, :rows, :] = jnp.where(kt == 0, part, acc[w, :rows, :] + part)
            return 0

        lax.fori_loop(0, x_buf.shape[-1] // k_tile, k_step, 0)
        for n, (bz, by, h) in enumerate(blocks):
            span = slice(n * half_rows, (n + 1) * half_rows)
            row = pl.ds(pl.multiple_of(((bz * SIDE + by) * 2 + h) * half_rows, half_rows), half_rows)
            q_buf[row, :] = acc[0, span, :].astype(jnp.bfloat16)
            k_new, v_new = acc[1, span, :].astype(jnp.bfloat16), acc[2, span, :].astype(jnp.bfloat16)
            stage[0, row, :head_dim] = k_new
            stage[0, row, head_dim:] = v_new
            kv_own[off + n * half_rows:off + (n + 1) * half_rows, :head_dim] = k_new
            kv_own[off + n * half_rows:off + (n + 1) * half_rows, head_dim:] = v_new
        spans[i] = (off, rows)

    def ring(delta):
        return at(x, delta) * 2 + core

    spans, kv_direct, kv_forward, pair_own, pair_side, pair_far = {}, {}, {}, [], [], []

    def kv_send(i):
        span = pl.ds(*spans[i])
        src, dst = kv_own.at[span], kv_hbm.at[cp, span]
        kv_direct[i] = start([remote(src, dst, cp=ring(1)), remote(src, dst, cp=ring(3))])
        pair_own.extend(start([remote(src, dst, cp=other)]))

    def kv_relay(i):
        off, rows = spans[i]
        arrived(kv_direct[i])
        up, down = kv_hbm.at[ring(3), pl.ds(off, rows // 2)], kv_hbm.at[ring(1), pl.ds(off + rows // 2, rows // 2)]
        kv_forward[i] = start([remote(up, up, cp=ring(1)), remote(down, down, cp=ring(3))])
        for d in (3, 1):
            ref = kv_hbm.at[ring(d), pl.ds(off, rows)]
            pair_side.extend(start([remote(ref, ref, cp=other)]))

    def kv_finish(i):
        arrived(kv_forward[i])
        ref = kv_hbm.at[ring(2), pl.ds(*spans[i])]
        pair_far.extend(start([remote(ref, ref, cp=other)]))

    xs.first()
    xs.second(0)
    ctp = start([remote(cnt_mine, cnt_tp.at[d - 1], tp=lax.rem(tp + d, n_tp)) for d in range(1, n_tp)])
    for c in load_w:
        c.wait()
    project(0)
    kv_send(0)
    xs.first_forward()
    xs.second(1)
    xs.second(3)
    project(1)
    kv_send(1)
    arrived(ctp)
    total = cnt_mine[...]
    for d in range(1, n_tp):
        total = total + cnt_tp[d - 1]
    cnt_row[...] = total
    kv_relay(0)
    xs.second_forward(0)
    project(2)
    kv_send(2)
    ccp = start([remote(cnt_row, cnt_cp.at[d - 1], cp=lax.rem(cp + d, n_cp)) for d in range(1, n_cp)])
    kv_relay(1)
    arrived(xs.f1)
    xs.second(2)
    kv_finish(0)
    xs.second_forward(1)
    project(3)
    kv_send(3)
    kv_relay(2)
    kv_finish(1)
    xs.second_forward(3)
    arrived(xs.f2[0])
    project(4)
    kv_send(4)
    kv_relay(3)
    kv_finish(2)
    xs.second_forward(2)
    for c in load_wo:
        c.wait()
    wq.first()
    wq.second(0)
    arrived(xs.f2[1])
    project(5)
    kv_send(5)
    kv_relay(4)
    kv_finish(3)
    arrived(xs.f2[3])
    arrived(xs.f2[2])
    project(6)
    kv_send(6)
    wq.first_forward()
    wq.second(1)
    wq.second(3)
    ws.first()
    ws.second(0)
    kv_relay(5)
    kv_finish(4)

    arrived(ccp)
    total = cnt_row[...]
    for d in range(1, n_cp):
        total = total + cnt_cp[d - 1]
    bounds = jnp.sum(total, axis=1, keepdims=True)
    n_part = 256

    def position(row0):
        late = lax.div(row0, piece)
        return (1 - late) * (cp * piece + row0) + late * ((n_pieces - 1 - cp) * piece + row0 - piece)

    def prepare(i, _):
        row0 = pl.multiple_of(i * n_part, n_part)
        pos = (position(row0) + lax.broadcasted_iota(jnp.int32, (n_part, 128), 0)).astype(jnp.float32)
        lo = jnp.zeros_like(pos)
        for d in range(N_DOCS):
            begin = jnp.broadcast_to(bounds[d:d + 1, :], pos.shape)
            lo = jnp.where(pos >= begin, jnp.maximum(lo, begin), lo)
        rows = pl.ds(row0, n_part)
        lo_buf[rows, :] = lo.astype(jnp.int32)
        m_buf[rows, :] = jnp.full((n_part, 128), NEG_BIG, jnp.float32)
        l_buf[rows, :] = jnp.zeros((n_part, 128), jnp.float32)
        o_acc[rows, :] = jnp.zeros((n_part, head_dim), jnp.float32)
        return 0

    lax.fori_loop(0, n_rows // n_part, prepare, 0)

    def attend(slot, row0, key_tile, pos_k0, causal):
        keys = pl.ds(pl.multiple_of(key_tile * piece, piece), piece)
        k_blk = stage[slot, keys, :head_dim]
        v_blk = stage[slot, keys, head_dim:]
        chains = [pl.ds(pl.multiple_of(row0 + c * CHAIN, CHAIN), CHAIN) for c in range(PAIR // CHAIN)]
        lane = lax.broadcasted_iota(jnp.int32, (CHAIN, piece), 1)
        wide_of = lambda v: jnp.tile(v, (1, piece // 128))
        scores = [lax.dot_general(q_buf[rows, :], k_blk, (((1,), (1,)), ((), ())), preferred_element_type=jnp.float32) for rows in chains]
        olds = [(m_buf[rows, :], l_buf[rows, :], o_acc[rows, :], lo_buf[rows, :]) for rows in chains]
        news = []
        for c, (s, (m_old, l_old, o_old, lo)) in enumerate(zip(scores, olds)):
            visible = lane >= wide_of(lo - pos_k0)
            if causal:
                pos_q = position(row0) + c * CHAIN - pos_k0 + lax.broadcasted_iota(jnp.int32, (CHAIN, 128), 0)
                visible = visible & (lane <= wide_of(pos_q))
            s = jnp.where(visible, s, NEG_BIG)
            m_new = jnp.maximum(m_old, jnp.max(s, axis=1, keepdims=True))
            alpha = jnp.exp2((m_old - m_new) * coef)
            p = jnp.exp2((s - wide_of(m_new)) * coef)
            l_new = alpha * l_old
            for i in range(piece // 128):
                l_new = l_new + p[:, i * 128:(i + 1) * 128]
            pv = jnp.dot(p.astype(jnp.bfloat16), v_blk, preferred_element_type=jnp.float32)
            news.append((m_new, l_new, o_old * jnp.tile(alpha, (1, head_dim // 128)) + pv))
        for rows, (m_new, l_new, o_new) in zip(chains, news):
            m_buf[rows, :] = m_new
            l_buf[rows, :] = l_new
            o_acc[rows, :] = o_new

    per_piece = piece // PAIR

    def diagonal(lo, hi):
        def step(u, _):
            key_tile = lax.div(u, 2 * per_piece)
            row0 = (u - key_tile * per_piece) * PAIR
            pos_k0 = (1 - key_tile) * cp * piece + key_tile * (n_pieces - 1 - cp) * piece
            attend(0, row0, key_tile, pos_k0, True)
            return 0
        lax.fori_loop(lo, hi, step, 0)

    def block_of(src, slot):
        earlier = lax.div(cp - src + n_cp - 1, n_cp)

        def step(u, _):
            key_tile = (1 - earlier) * lax.div(u, per_piece)
            row0 = (earlier * u + (1 - earlier) * (per_piece + lax.rem(u, per_piece))) * PAIR
            pos_k0 = (1 - key_tile) * src * piece + key_tile * (n_pieces - 1 - src) * piece
            attend(slot, row0, key_tile, pos_k0, False)
            return 0
        lax.fori_loop(0, 2 * per_piece, step, 0)

    def fetch(src, slot):
        copies = []
        for n, (dz, dy, h) in enumerate(ORDER):
            row = pl.multiple_of(((at(z, dz) * SIDE + at(y, dy)) * 2 + h) * half_rows, half_rows)
            copies.append(pltpu.make_async_copy(kv_hbm.at[src, pl.ds(n * half_rows, half_rows)], stage.at[slot, pl.ds(row, half_rows)], stage_sem.at[slot]))
        for c in copies:
            c.start()
        return pltpu.make_async_copy(kv_hbm.at[src], stage.at[slot], stage_sem.at[slot])

    def landed(whole):
        whole.wait()

    n_diag = 3 * per_piece
    wx_direct, wx_forward = [], []

    def wo_along_x():
        for da in (0, 1, 3, 2):
            arrived(wq.f2[da])
        low, high = [wx_buf.at[x, pl.ds(lo, SIDE // 2)] for lo in (0, SIDE // 2)]
        wx_direct.extend(start([remote(low, low, cp=ring(1)), remote(high, high, cp=ring(3)),
                                remote(high, high, cp=ring(1)), remote(low, low, cp=ring(3))]))

    def wo_relay_x():
        arrived(wx_direct[:2])
        up, down = wx_buf.at[at(x, 3), pl.ds(0, SIDE // 2)], wx_buf.at[at(x, 1), pl.ds(SIDE // 2, SIDE // 2)]
        wx_forward.extend(start([remote(up, up, cp=ring(1)), remote(down, down, cp=ring(3))]))

    diagonal(0, n_diag // 3)
    wq.second_forward(0)
    arrived(wq.f1)
    wq.second(2)
    kv_relay(6)
    kv_finish(5)
    wq.second_forward(1)
    wq.second_forward(3)
    diagonal(n_diag // 3, 2 * n_diag // 3)
    wq.second_forward(2)
    ws.first_forward()
    ws.second(1)
    ws.second(3)
    arrived(pair_own)
    now = fetch(other, 1)
    kv_finish(6)
    diagonal(2 * n_diag // 3, n_diag)
    wo_along_x()
    ws.second_forward(0)

    def near(d, mine):
        return at(x, d) * 2 + (core if mine else 1 - core)

    landed(now)
    now = fetch(near(3, True), 0)
    block_of(other, 1)
    arrived(ws.f1)
    ws.second(2)
    landed(now)
    now = fetch(near(1, True), 1)
    block_of(near(3, True), 0)
    ws.second_forward(1)
    arrived(pair_side)
    landed(now)
    now = fetch(near(3, False), 0)
    block_of(near(1, True), 1)
    wo_relay_x()
    ws.second_forward(3)
    landed(now)
    now = fetch(near(1, False), 1)
    block_of(near(3, False), 0)
    arrived(pair_far)
    landed(now)
    now = fetch(near(2, True), 0)
    block_of(near(1, False), 1)
    ws.second_forward(2)
    landed(now)
    now = fetch(near(2, False), 1)
    block_of(near(2, True), 0)
    landed(now)
    block_of(near(2, False), 1)

    def finish(i, _):
        rows = pl.ds(pl.multiple_of(i * 128, 128), 128)
        o_mine[i] = (o_acc[rows, :] / jnp.sum(l_buf[rows, :], axis=1, keepdims=True)).astype(jnp.bfloat16)
        return 0

    lax.fori_loop(0, n_tp, finish, 0)
    turns = (2, 1, 3, 0)
    o_sent = {}
    for dz in turns:
        for dy in turns:
            if dz or dy:
                peer = at(z, dz) * SIDE + at(y, dy)
                o_sent[dz, dy] = start([remote(o_mine.at[peer], o_all.at[tp, 0], tp=peer)])
    o_pair = {(0, 0): start([remote(o_mine.at[tp], o_all.at[tp, 1], cp=other)])}
    o_all[tp, 0] = o_mine[tp]
    for da in (0, 1, 3, 2):
        arrived(ws.f2[da])
    arrived(wx_direct[2:])
    arrived(wx_forward)

    def pass_on(dz):
        for dy in turns:
            if dz or dy:
                arrived(o_sent[dz, dy])
                src = at(z, SIDE - dz) * SIDE + at(y, SIDE - dy)
                o_pair[dz, dy] = start([remote(o_all.at[src, 0], o_all.at[src, 1], cp=other)])

    def accumulate(turn, dz):
        for dy in turns:
            arrived(o_pair[dz, dy])
        zz = at(z, SIDE - dz)

        lhs = jnp.concatenate([o_all[zz * SIDE + yy].reshape(2 * o_mine.shape[1], head_dim) for yy in range(SIDE)], axis=1)

        def add(cols, rhs):
            part = jnp.dot(lhs, rhs, preferred_element_type=jnp.float32)
            if turn == 0:
                y_acc[:, cols] = part
            elif turn == SIDE - 1:
                y_out[:, cols] = (y_acc[:, cols] + part).astype(jnp.bfloat16)
            else:
                y_acc[:, cols] = y_acc[:, cols] + part

        for j in range(n_plane // 512):
            cols = pl.ds(j * 512, 512)
            add(cols, wo_buf[zz, :, :, :, cols].reshape(SIDE * head_dim, 512))
        add(pl.ds(n_plane, SIDE * n_quarter), jnp.concatenate([wx_buf[xx, zz].reshape(SIDE * head_dim, n_quarter) for xx in range(SIDE)], axis=1))

    pass_on(turns[0])
    for turn, dz in enumerate(turns):
        if turn + 1 < SIDE:
            pass_on(turns[turn + 1])
        accumulate(turn, dz)
    rows = o_mine.shape[1]
    cols = pl.ds(pl.multiple_of(core * wide, wide), wide)
    keep = pltpu.make_async_copy(y_out.at[pl.ds(0, rows)], y_hbm.at[:, cols], loc_sem.at[6])
    keep.start()
    y_pair = start([remote(y_out.at[pl.ds(rows, rows)], y_hbm.at[:, cols], cp=other)])
    arrived(y_pair)
    keep.wait()
    for c in sent:
        c.wait_send()


N_REMOTE = 3 * 40 + 6 + 7 * 8 + 15 + 7 + 15 + 16 + 1
CHAIN = 512
PAIR = 1024


def solution(mesh):
    def per_device(x_loc, seg_loc, w_q, w_k, w_v, w_o):
        rows, depth = x_loc.shape
        head_dim = w_q.shape[-1]
        half = rows // 2
        n_tp, n_cp = SIDE * SIDE, 2 * SIDE
        n_rows = n_tp * rows
        wide = w_o.shape[-1] // 2
        most = max(len(b) for b in BATCHES) * half
        hbm = pl.BlockSpec(memory_space=pltpu.HBM)
        f32, bf16 = jnp.float32, jnp.bfloat16
        dma, vmem = pltpu.SemaphoreType.DMA, pltpu.VMEM
        y_loc, _ = pl.pallas_call(
            attention_kernel,
            out_shape=(jax.ShapeDtypeStruct((rows, depth), bf16), jax.ShapeDtypeStruct((n_cp, n_rows, 2 * head_dim), bf16)),
            in_specs=[hbm, pl.BlockSpec(memory_space=vmem), hbm, hbm, hbm, hbm],
            out_specs=(hbm, hbm),
            scratch_shapes=[vmem((SIDE, SIDE, 2, half, depth), bf16), vmem((3, depth, head_dim), bf16),
                            vmem((n_rows, 2 * head_dim), bf16), vmem((3, most, head_dim), f32),
                            vmem((n_rows, head_dim), bf16), vmem((2, n_rows, 2 * head_dim), bf16),
                            vmem((n_rows, 128), f32), vmem((n_rows, 128), f32), vmem((n_rows, head_dim), f32),
                            vmem((n_rows, 128), jnp.int32), vmem((SIDE, SIDE, 2, head_dim // 2, wide // 3 * 2), bf16),
                            vmem((SIDE, SIDE, SIDE, 2, head_dim // 2, wide // 3 // SIDE), bf16),
                            vmem((n_tp, rows, head_dim), bf16), vmem((n_tp, 2, rows, head_dim), bf16),
                            vmem((2 * rows, wide), f32), vmem((2 * rows, wide), bf16),
                            vmem((8, rows), f32), vmem((n_tp - 1, 8, rows), f32), vmem((8, rows), f32), vmem((n_cp - 1, 8, rows), f32),
                            dma((N_REMOTE,)), dma((N_REMOTE,)), dma((7,)), dma((2,))],
            compiler_params=pltpu.CompilerParams(collective_id=0, has_side_effects=True, vmem_limit_bytes=63 * 2**20),
            cost_estimate=pl.CostEstimate(flops=40 * 10**9, bytes_accessed=30 * 10**6, transcendentals=0),
            name="packed_attention",
        )(x_loc.reshape(2, half, depth), seg_loc.reshape(1, rows), w_q.reshape(depth, head_dim), w_k.reshape(depth, head_dim),
          w_v.reshape(depth, head_dim), w_o.reshape(2, head_dim // 2, 2 * wide))
        return y_loc

    return jax.shard_map(
        per_device, mesh=mesh,
        in_specs=(P(("dp", "cp", "tp"), None), P(("dp", "cp", "tp")), P(None, "tp", None), P(None, "tp", None), P(None, "tp", None), P("tp", None, None)),
        out_specs=P(("dp", "cp", "tp"), None), check_vma=False)
```

```python
import jax
import jax.numpy as jnp
from jax import lax
from jax.experimental import pallas as pl
from jax.experimental.pallas import tpu as pltpu
from jax.sharding import PartitionSpec as P

NEG_BIG = -1e30
LOG2E = 1.4426950408889634
N_DOCS = 6
SIDE = 4
MESH = pl.DeviceIdType.MESH

BATCHES = (
    ((0, 0, 0), (0, 0, 1)),
    ((0, 1, 0), (0, 3, 0), (1, 0, 1), (3, 0, 1)),
    ((1, 0, 0), (3, 0, 0), (0, 1, 1), (0, 3, 1)),
    ((0, 2, 0), (2, 0, 1), (1, 1, 0), (3, 1, 0), (1, 1, 1), (1, 3, 1)),
    ((1, 3, 0), (3, 3, 0), (3, 1, 1), (3, 3, 1), (2, 0, 0), (0, 2, 1)),
    ((1, 2, 0), (3, 2, 0), (2, 1, 1), (2, 3, 1), (2, 1, 0), (1, 2, 1)),
    ((2, 3, 0), (3, 2, 1), (2, 2, 0), (2, 2, 1)),
)
ORDER = tuple(blk for batch in BATCHES for blk in batch)


def attention_kernel(x_hbm, seg_ref, wq_hbm, wk_hbm, wv_hbm, wo_hbm, y_hbm, kv_hbm,
                     x_buf, w_buf, kv_own, acc, q_buf, stage, m_buf, l_buf, o_acc, lo_buf, wo_buf, wx_buf, o_mine, o_all, y_acc, y_out,
                     cnt_mine, cnt_tp, cnt_row, cnt_cp, send_sem, recv_sem, loc_sem, stage_sem):
    tp, cp = lax.axis_index("tp"), lax.axis_index("cp")
    n_tp, n_cp = SIDE * SIDE, 2 * SIDE
    z, y = lax.div(tp, SIDE), lax.rem(tp, SIDE)
    x, core = lax.div(cp, 2), lax.rem(cp, 2)
    other = x * 2 + 1 - core
    half_rows = x_buf.shape[3]
    head_dim = q_buf.shape[-1]
    n_rows = q_buf.shape[0]
    piece = n_rows // 2
    n_pieces = 2 * n_cp
    n_plane, n_quarter = wo_buf.shape[-1], wx_buf.shape[-1]
    wide = n_plane + SIDE * n_quarter
    coef = LOG2E * head_dim ** -0.5
    k_tile = 768
    n_used = [0]

    def at(pos, delta):
        return lax.rem(pos + delta, SIDE)

    def remote(src, dst, **device):
        idx = n_used[0]
        n_used[0] += 1
        return pltpu.make_async_remote_copy(src_ref=src, dst_ref=dst, send_sem=send_sem.at[idx], recv_sem=recv_sem.at[idx],
                                            device_id=device, device_id_type=MESH)

    sent = []

    def start(copies):
        for c in copies:
            c.start()
            sent.append(c)
        return copies

    def arrived(copies):
        for c in copies:
            c.wait_recv()

    load_x = pltpu.make_async_copy(x_hbm, x_buf.at[z, y], loc_sem.at[0])
    load_x.start()
    load_w = [pltpu.make_async_copy(w, w_buf.at[i], loc_sem.at[1 + i]) for i, w in enumerate((wq_hbm, wk_hbm, wv_hbm))]
    for c in load_w:
        c.start()
    load_wo = [pltpu.make_async_copy(wo_hbm.at[:, :, pl.ds(pl.multiple_of(core * wide + first, n_quarter), size)], dst, loc_sem.at[4 + i])
               for i, (first, size, dst) in enumerate(((0, n_plane, wo_buf.at[z, y]), (n_plane + x * n_quarter, n_quarter, wx_buf.at[x, z, y])))]
    for c in load_wo:
        c.start()
    cnt_mine[...] = (seg_ref[...] < lax.broadcasted_iota(jnp.int32, cnt_mine.shape, 0)).astype(jnp.float32)

    barrier = pltpu.get_barrier_semaphore()
    for d in range(1, n_tp):
        pl.semaphore_signal(barrier, inc=1, device_id={"tp": lax.rem(tp + d, n_tp)}, device_id_type=MESH)
    for d in range(1, n_cp):
        pl.semaphore_signal(barrier, inc=1, device_id={"cp": lax.rem(cp + d, n_cp)}, device_id_type=MESH)
    pl.semaphore_wait(barrier, n_tp - 1 + n_cp - 1)
    load_x.wait()

    def device_a(fam, delta):
        return z * SIDE + at(y, delta) if fam == 0 else at(z, delta) * SIDE + y

    def device_b(fam, delta):
        return device_a(1 - fam, delta)

    class Plane:
        def __init__(self, buf):
            self.buf = buf
            self.rows = buf.shape[3]
            self.s1, self.f1, self.s2, self.f2 = [], [], {}, {}

        def block(self, fam, b, a, part=None):
            half = self.rows // 2
            rows = pl.ds(0, self.rows) if part is None else pl.ds(part * half, half)
            return self.buf.at[b, a, 0, rows] if fam == 0 else self.buf.at[a, b, 1, rows]

        def first(self):
            for fam, (a, b) in enumerate(((y, z), (z, y))):
                src = self.block(fam, b, a)
                self.s1 += start([remote(src, src, tp=device_a(fam, d)) for d in (1, 3)])

        def first_forward(self):
            arrived(self.s1)
            for fam, (a, b) in enumerate(((y, z), (z, y))):
                up, down = self.block(fam, b, at(a, 3), 0), self.block(fam, b, at(a, 1), 1)
                self.f1 += start([remote(up, up, tp=device_a(fam, 1)), remote(down, down, tp=device_a(fam, 3))])

        def second(self, da):
            self.s2[da] = []
            for fam, (a, b) in enumerate(((y, z), (z, y))):
                src = self.block(fam, b, at(a, da))
                self.s2[da] += start([remote(src, src, tp=device_b(fam, d)) for d in (1, 3)])

        def second_forward(self, da):
            arrived(self.s2[da])
            self.f2[da] = []
            for fam, (a, b) in enumerate(((y, z), (z, y))):
                up, down = self.block(fam, at(b, 3), at(a, da), 0), self.block(fam, at(b, 1), at(a, da), 1)
                self.f2[da] += start([remote(up, up, tp=device_b(fam, 1)), remote(down, down, tp=device_b(fam, 3))])

    xs, ws, wq = Plane(x_buf), Plane(wo_buf), Plane(wx_buf.at[x])

    def project(i):
        blocks = [(at(z, dz), at(y, dy), h) for dz, dy, h in BATCHES[i]]
        rows = len(blocks) * half_rows
        off = sum(len(b) for b in BATCHES[:i]) * half_rows

        def k_step(kt, _):
            cols = pl.ds(pl.multiple_of(kt * k_tile, k_tile), k_tile)
            lhs = jnp.concatenate([x_buf[bz, by, h, :, cols] for bz, by, h in blocks], axis=0)
            for w in range(3):
                part = jnp.dot(lhs, w_buf[w, cols, :], preferred_element_type=jnp.float32)
                acc[w, :rows, :] = jnp.where(kt == 0, part, acc[w, :rows, :] + part)
            return 0

        lax.fori_loop(0, x_buf.shape[-1] // k_tile, k_step, 0)
        for n, (bz, by, h) in enumerate(blocks):
            span = slice(n * half_rows, (n + 1) * half_rows)
            row = pl.ds(pl.multiple_of(((bz * SIDE + by) * 2 + h) * half_rows, half_rows), half_rows)
            q_buf[row, :] = acc[0, span, :].astype(jnp.bfloat16)
            k_new, v_new = acc[1, span, :].astype(jnp.bfloat16), acc[2, span, :].astype(jnp.bfloat16)
            stage[0, row, :head_dim] = k_new
            stage[0, row, head_dim:] = v_new
            kv_own[off + n * half_rows:off + (n + 1) * half_rows, :head_dim] = k_new
            kv_own[off + n * half_rows:off + (n + 1) * half_rows, head_dim:] = v_new
        spans[i] = (off, rows)

    def ring(delta):
        return at(x, delta) * 2 + core

    spans, kv_direct, kv_forward, pair_own, pair_side, pair_far = {}, {}, {}, [], [], []

    def kv_send(i):
        span = pl.ds(*spans[i])
        src, dst = kv_own.at[span], kv_hbm.at[cp, span]
        kv_direct[i] = start([remote(src, dst, cp=ring(1)), remote(src, dst, cp=ring(3))])
        pair_own.extend(start([remote(src, dst, cp=other)]))

    def kv_relay(i):
        off, rows = spans[i]
        arrived(kv_direct[i])
        up, down = kv_hbm.at[ring(3), pl.ds(off, rows // 2)], kv_hbm.at[ring(1), pl.ds(off + rows // 2, rows // 2)]
        kv_forward[i] = start([remote(up, up, cp=ring(1)), remote(down, down, cp=ring(3))])
        for d in (3, 1):
            ref = kv_hbm.at[ring(d), pl.ds(off, rows)]
            pair_side.extend(start([remote(ref, ref, cp=other)]))

    def kv_finish(i):
        arrived(kv_forward[i])
        ref = kv_hbm.at[ring(2), pl.ds(*spans[i])]
        pair_far.extend(start([remote(ref, ref, cp=other)]))

    xs.first()
    xs.second(0)
    ctp = start([remote(cnt_mine, cnt_tp.at[d - 1], tp=lax.rem(tp + d, n_tp)) for d in range(1, n_tp)])
    for c in load_w:
        c.wait()
    project(0)
    kv_send(0)
    xs.first_forward()
    xs.second(1)
    xs.second(3)
    project(1)
    kv_send(1)
    arrived(ctp)
    total = cnt_mine[...]
    for d in range(1, n_tp):
        total = total + cnt_tp[d - 1]
    cnt_row[...] = total
    kv_relay(0)
    xs.second_forward(0)
    project(2)
    kv_send(2)
    ccp = start([remote(cnt_row, cnt_cp.at[d - 1], cp=lax.rem(cp + d, n_cp)) for d in range(1, n_cp)])
    kv_relay(1)
    arrived(xs.f1)
    xs.second(2)
    kv_finish(0)
    xs.second_forward(1)
    project(3)
    kv_send(3)
    kv_relay(2)
    kv_finish(1)
    xs.second_forward(3)
    arrived(xs.f2[0])
    project(4)
    kv_send(4)
    kv_relay(3)
    kv_finish(2)
    xs.second_forward(2)
    for c in load_wo:
        c.wait()
    wq.first()
    wq.second(0)
    arrived(xs.f2[1])
    project(5)
    kv_send(5)
    kv_relay(4)
    kv_finish(3)
    arrived(xs.f2[3])
    arrived(xs.f2[2])
    project(6)
    kv_send(6)
    wq.first_forward()
    wq.second(1)
    wq.second(3)
    ws.first()
    ws.second(0)
    kv_relay(5)
    kv_finish(4)

    arrived(ccp)
    total = cnt_row[...]
    for d in range(1, n_cp):
        total = total + cnt_cp[d - 1]
    bounds = jnp.sum(total, axis=1, keepdims=True)
    n_part = 256

    def position(row0):
        late = lax.div(row0, piece)
        return (1 - late) * (cp * piece + row0) + late * ((n_pieces - 1 - cp) * piece + row0 - piece)

    def prepare(i, _):
        row0 = pl.multiple_of(i * n_part, n_part)
        pos = (position(row0) + lax.broadcasted_iota(jnp.int32, (n_part, 128), 0)).astype(jnp.float32)
        lo = jnp.zeros_like(pos)
        for d in range(N_DOCS):
            begin = jnp.broadcast_to(bounds[d:d + 1, :], pos.shape)
            lo = jnp.where(pos >= begin, jnp.maximum(lo, begin), lo)
        rows = pl.ds(row0, n_part)
        lo_buf[rows, :] = lo.astype(jnp.int32)
        m_buf[rows, :] = jnp.full((n_part, 128), NEG_BIG, jnp.float32)
        l_buf[rows, :] = jnp.zeros((n_part, 128), jnp.float32)
        o_acc[rows, :] = jnp.zeros((n_part, head_dim), jnp.float32)
        return 0

    lax.fori_loop(0, n_rows // n_part, prepare, 0)

    def attend(slot, row0, key_tile, pos_k0, causal):
        keys = pl.ds(pl.multiple_of(key_tile * piece, piece), piece)
        k_blk = stage[slot, keys, :head_dim]
        v_blk = stage[slot, keys, head_dim:]
        chains = [pl.ds(pl.multiple_of(row0 + c * CHAIN, CHAIN), CHAIN) for c in range(PAIR // CHAIN)]
        lane = lax.broadcasted_iota(jnp.int32, (CHAIN, piece), 1)
        wide_of = lambda v: jnp.tile(v, (1, piece // 128))
        scores = [lax.dot_general(q_buf[rows, :], k_blk, (((1,), (1,)), ((), ())), preferred_element_type=jnp.float32) for rows in chains]
        olds = [(m_buf[rows, :], l_buf[rows, :], o_acc[rows, :], lo_buf[rows, :]) for rows in chains]
        news = []
        for c, (s, (m_old, l_old, o_old, lo)) in enumerate(zip(scores, olds)):
            visible = lane >= wide_of(lo - pos_k0)
            if causal:
                pos_q = position(row0) + c * CHAIN - pos_k0 + lax.broadcasted_iota(jnp.int32, (CHAIN, 128), 0)
                visible = visible & (lane <= wide_of(pos_q))
            s = jnp.where(visible, s, NEG_BIG)
            m_new = jnp.maximum(m_old, jnp.max(s, axis=1, keepdims=True))
            alpha = jnp.exp2((m_old - m_new) * coef)
            p = jnp.exp2((s - wide_of(m_new)) * coef)
            l_new = alpha * l_old
            for i in range(piece // 128):
                l_new = l_new + p[:, i * 128:(i + 1) * 128]
            pv = jnp.dot(p.astype(jnp.bfloat16), v_blk, preferred_element_type=jnp.float32)
            news.append((m_new, l_new, o_old * jnp.tile(alpha, (1, head_dim // 128)) + pv))
        for rows, (m_new, l_new, o_new) in zip(chains, news):
            m_buf[rows, :] = m_new
            l_buf[rows, :] = l_new
            o_acc[rows, :] = o_new

    per_piece = piece // PAIR

    def diagonal(lo, hi):
        def step(u, _):
            key_tile = lax.div(u, 2 * per_piece)
            row0 = (u - key_tile * per_piece) * PAIR
            pos_k0 = (1 - key_tile) * cp * piece + key_tile * (n_pieces - 1 - cp) * piece
            attend(0, row0, key_tile, pos_k0, True)
            return 0
        lax.fori_loop(lo, hi, step, 0)

    def block_of(src, slot, lo=0, hi=None):
        earlier = lax.div(cp - src + n_cp - 1, n_cp)

        def step(u, _):
            key_tile = (1 - earlier) * lax.div(u, per_piece)
            row0 = (earlier * u + (1 - earlier) * (per_piece + lax.rem(u, per_piece))) * PAIR
            pos_k0 = (1 - key_tile) * src * piece + key_tile * (n_pieces - 1 - src) * piece
            attend(slot, row0, key_tile, pos_k0, False)
            return 0
        lax.fori_loop(lo, 2 * per_piece if hi is None else hi, step, 0)

    def fetch(src, slot):
        copies = []
        for n, (dz, dy, h) in enumerate(ORDER):
            row = pl.multiple_of(((at(z, dz) * SIDE + at(y, dy)) * 2 + h) * half_rows, half_rows)
            copies.append(pltpu.make_async_copy(kv_hbm.at[src, pl.ds(n * half_rows, half_rows)], stage.at[slot, pl.ds(row, half_rows)], stage_sem.at[slot]))
        for c in copies:
            c.start()
        return pltpu.make_async_copy(kv_hbm.at[src], stage.at[slot], stage_sem.at[slot])

    def landed(whole):
        whole.wait()

    n_diag = 3 * per_piece
    wx_direct, wx_forward = [], []

    def wo_along_x():
        for da in (0, 1, 3, 2):
            arrived(wq.f2[da])
        low, high = [wx_buf.at[x, pl.ds(lo, SIDE // 2)] for lo in (0, SIDE // 2)]
        wx_direct.extend(start([remote(low, low, cp=ring(1)), remote(high, high, cp=ring(3)),
                                remote(high, high, cp=ring(1)), remote(low, low, cp=ring(3))]))

    def wo_relay_x():
        arrived(wx_direct[:2])
        up, down = wx_buf.at[at(x, 3), pl.ds(0, SIDE // 2)], wx_buf.at[at(x, 1), pl.ds(SIDE // 2, SIDE // 2)]
        wx_forward.extend(start([remote(up, up, cp=ring(1)), remote(down, down, cp=ring(3))]))

    diagonal(0, n_diag // 3)
    wq.second_forward(0)
    arrived(wq.f1)
    wq.second(2)
    kv_relay(6)
    kv_finish(5)
    wq.second_forward(1)
    wq.second_forward(3)
    diagonal(n_diag // 3, 2 * n_diag // 3)
    wq.second_forward(2)
    ws.first_forward()
    ws.second(1)
    ws.second(3)
    arrived(pair_own)
    now = fetch(other, 1)
    kv_finish(6)
    diagonal(2 * n_diag // 3, n_diag)
    wo_along_x()
    ws.second_forward(0)

    def near(d, mine):
        return at(x, d) * 2 + (core if mine else 1 - core)

    landed(now)
    now = fetch(near(3, True), 0)
    block_of(other, 1)
    arrived(ws.f1)
    ws.second(2)
    landed(now)
    now = fetch(near(1, True), 1)
    block_of(near(3, True), 0)
    ws.second_forward(1)
    arrived(pair_side)
    landed(now)
    now = fetch(near(3, False), 0)
    block_of(near(1, True), 1)
    wo_relay_x()
    ws.second_forward(3)
    landed(now)
    now = fetch(near(1, False), 1)
    block_of(near(3, False), 0)
    arrived(pair_far)
    landed(now)
    now = fetch(near(2, True), 0)
    block_of(near(1, False), 1)
    ws.second_forward(2)
    landed(now)
    now = fetch(near(2, False), 1)
    block_of(near(2, True), 0, 0, per_piece)
    landed(now)
    block_of(near(2, False), 1, 0, per_piece)

    def finish(i, _):
        rows = pl.ds(pl.multiple_of(i * 128, 128), 128)
        o_mine[i] = (o_acc[rows, :] / jnp.sum(l_buf[rows, :], axis=1, keepdims=True)).astype(jnp.bfloat16)
        return 0

    turns = (2, 1, 3, 0)
    o_sent = {}
    for dz in turns:
        for dy in turns:
            if dz or dy:
                peer = at(z, dz) * SIDE + at(y, dy)
                o_sent[dz, dy] = [remote(o_mine.at[peer], o_all.at[tp, 0], tp=peer)]
                sent.extend(o_sent[dz, dy])

    def hand_out(late):
        for dz in turns:
            @pl.when(lax.div(at(z, dz), SIDE // 2) == late)
            def _():
                for dy in turns:
                    if dz or dy:
                        o_sent[dz, dy][0].start()

    lax.fori_loop(0, n_tp // 2, finish, 0)
    hand_out(0)
    block_of(near(2, True), 0, per_piece, 2 * per_piece)
    block_of(near(2, False), 1, per_piece, 2 * per_piece)
    lax.fori_loop(n_tp // 2, n_tp, finish, 0)
    hand_out(1)
    o_pair = {(0, 0): start([remote(o_mine.at[tp], o_all.at[tp, 1], cp=other)])}
    o_all[tp, 0] = o_mine[tp]
    for da in (0, 1, 3, 2):
        arrived(ws.f2[da])
    arrived(wx_direct[2:])
    arrived(wx_forward)

    def pass_on(dz):
        for dy in turns:
            if dz or dy:
                arrived(o_sent[dz, dy])
                src = at(z, SIDE - dz) * SIDE + at(y, SIDE - dy)
                o_pair[dz, dy] = start([remote(o_all.at[src, 0], o_all.at[src, 1], cp=other)])

    def accumulate(turn, dz):
        for dy in turns:
            arrived(o_pair[dz, dy])
        zz = at(z, SIDE - dz)

        lhs = jnp.concatenate([o_all[zz * SIDE + yy].reshape(2 * o_mine.shape[1], head_dim) for yy in range(SIDE)], axis=1)

        def add(cols, rhs):
            part = jnp.dot(lhs, rhs, preferred_element_type=jnp.float32)
            if turn == 0:
                y_acc[:, cols] = part
            elif turn == SIDE - 1:
                y_out[:, cols] = (y_acc[:, cols] + part).astype(jnp.bfloat16)
            else:
                y_acc[:, cols] = y_acc[:, cols] + part

        for j in range(n_plane // 512):
            cols = pl.ds(j * 512, 512)
            add(cols, wo_buf[zz, :, :, :, cols].reshape(SIDE * head_dim, 512))
        add(pl.ds(n_plane, SIDE * n_quarter), jnp.concatenate([wx_buf[xx, zz].reshape(SIDE * head_dim, n_quarter) for xx in range(SIDE)], axis=1))

    pass_on(turns[0])
    for turn, dz in enumerate(turns):
        if turn + 1 < SIDE:
            pass_on(turns[turn + 1])
        accumulate(turn, dz)
    rows = o_mine.shape[1]
    cols = pl.ds(pl.multiple_of(core * wide, wide), wide)
    keep = pltpu.make_async_copy(y_out.at[pl.ds(0, rows)], y_hbm.at[:, cols], loc_sem.at[6])
    keep.start()
    y_pair = start([remote(y_out.at[pl.ds(rows, rows)], y_hbm.at[:, cols], cp=other)])
    arrived(y_pair)
    keep.wait()
    for c in sent:
        c.wait_send()


N_REMOTE = 3 * 40 + 6 + 7 * 8 + 15 + 7 + 15 + 16 + 1
CHAIN = 512
PAIR = 1024


def solution(mesh):
    def per_device(x_loc, seg_loc, w_q, w_k, w_v, w_o):
        rows, depth = x_loc.shape
        head_dim = w_q.shape[-1]
        half = rows // 2
        n_tp, n_cp = SIDE * SIDE, 2 * SIDE
        n_rows = n_tp * rows
        wide = w_o.shape[-1] // 2
        most = max(len(b) for b in BATCHES) * half
        hbm = pl.BlockSpec(memory_space=pltpu.HBM)
        f32, bf16 = jnp.float32, jnp.bfloat16
        dma, vmem = pltpu.SemaphoreType.DMA, pltpu.VMEM
        y_loc, _ = pl.pallas_call(
            attention_kernel,
            out_shape=(jax.ShapeDtypeStruct((rows, depth), bf16), jax.ShapeDtypeStruct((n_cp, n_rows, 2 * head_dim), bf16)),
            in_specs=[hbm, pl.BlockSpec(memory_space=vmem), hbm, hbm, hbm, hbm],
            out_specs=(hbm, hbm),
            scratch_shapes=[vmem((SIDE, SIDE, 2, half, depth), bf16), vmem((3, depth, head_dim), bf16),
                            vmem((n_rows, 2 * head_dim), bf16), vmem((3, most, head_dim), f32),
                            vmem((n_rows, head_dim), bf16), vmem((2, n_rows, 2 * head_dim), bf16),
                            vmem((n_rows, 128), f32), vmem((n_rows, 128), f32), vmem((n_rows, head_dim), f32),
                            vmem((n_rows, 128), jnp.int32), vmem((SIDE, SIDE, 2, head_dim // 2, wide // 3 * 2), bf16),
                            vmem((SIDE, SIDE, SIDE, 2, head_dim // 2, wide // 3 // SIDE), bf16),
                            vmem((n_tp, rows, head_dim), bf16), vmem((n_tp, 2, rows, head_dim), bf16),
                            vmem((2 * rows, wide), f32), vmem((2 * rows, wide), bf16),
                            vmem((8, rows), f32), vmem((n_tp - 1, 8, rows), f32), vmem((8, rows), f32), vmem((n_cp - 1, 8, rows), f32),
                            dma((N_REMOTE,)), dma((N_REMOTE,)), dma((7,)), dma((2,))],
            compiler_params=pltpu.CompilerParams(collective_id=0, has_side_effects=True, vmem_limit_bytes=63 * 2**20),
            cost_estimate=pl.CostEstimate(flops=40 * 10**9, bytes_accessed=30 * 10**6, transcendentals=0),
            name="packed_attention",
        )(x_loc.reshape(2, half, depth), seg_loc.reshape(1, rows), w_q.reshape(depth, head_dim), w_k.reshape(depth, head_dim),
          w_v.reshape(depth, head_dim), w_o.reshape(2, head_dim // 2, 2 * wide))
        return y_loc

    return jax.shard_map(
        per_device, mesh=mesh,
        in_specs=(P(("dp", "cp", "tp"), None), P(("dp", "cp", "tp")), P(None, "tp", None), P(None, "tp", None), P(None, "tp", None), P("tp", None, None)),
        out_specs=P(("dp", "cp", "tp"), None), check_vma=False)
```
